512 devices in a mesh: pair: 2 (over y_lo), dp: 32 (over x, z), ep: 8 (over y_hi, core).
Axes of the slice: x: 4, y: 8 (y_hi: 4, y_lo: 2; y = y_hi * 2 + y_lo), z: 8, core: 2. Of those that a mesh axis runs over, the one named last changes fastest.
Arguments:
- activations: bfloat16 [49152, 4096], P(('pair', 'dp'), 'ep'), parts along dimension 1, may hold values from -16 to 16
- cotangents: bfloat16 [49152, 16384], P(('pair', 'dp'), 'ep'), parts along dimension 1, may hold values from -1.75 to 1.75
Outputs:
- averaged_grad: bfloat16 [512, 16384], P('pair', 'ep'), parts along dimension 1
The draws below stay inside these ranges and needn't reach their ends.
There are 8 independent parts, one for each index of `ep`. The reference program is written for one: setup_inputs(seed, part) draws one part's arguments, and reference() takes and returns one part's arrays. A program takes and returns all parts, laid end to end along the dimension named above; each array names one. Nothing has to cross between parts.
All inputs are finite; a program needn't handle non-finite values.
Results may differ from the reference program's by a relative error of at most 0.001.
Values may be sent and summed in bfloat16 or wider, within the bound.
No kernel may reach another device: no remote copies, remote signals or barrier semaphores. Data moves between devices by JAX's collectives and lax.ppermute only.
A program may use at most 64 MiB of HBM per device.

```python
import jax
import jax.numpy as jnp

FF = 2048
ROWS = 512
TOK_DEV = 768
REPLICAS = 64
TOKENS = 49152
N_PAIR = 2
N_DP = 32


def raised(drawn, stream_key, source, target, parts, factor):
    def block_of(position):
        return (jnp.arange(drawn.shape[position]) // (drawn.shape[position] // parts)).reshape((-1,) + (1,) * (drawn.ndim - 1 - position))

    near = jax.random.permutation(stream_key, parts)[block_of(target)]
    second = (block_of(target) + parts // 2) % parts
    return jnp.where((block_of(source) == near) | (block_of(source) == second), factor * drawn, drawn)


def steps_of(own_key, extent, cuts, least, largest):
    def one(position, parts):
        draws = jax.random.uniform(jax.random.fold_in(jax.random.fold_in(own_key, 6), position), (parts,), jnp.float32, least / len(cuts), largest / len(cuts))
        return jnp.repeat(jnp.exp(draws), extent[position] // parts).reshape((-1,) + (1,) * (len(extent) - position - 1))

    factor_of = one(*cuts[0])
    for cut in cuts[1:]:
        factor_of = factor_of * one(*cut)
    return factor_of


def scatter_about(key, shape, scale, bound, cuts=(), held_as=jnp.bfloat16):
    entries = jax.random.normal(key, shape, jnp.float32) * scale
    if len(cuts) > 0:
        entries = steps_of(key, shape, cuts, -0.22, 0.18) * entries
    return jnp.clip(entries, min=-bound, max=bound).astype(held_as)


def gaussian_with(own_key, dims, scale, limit, cuts, heavy, held_as=jnp.bfloat16):
    drawn = scale * jax.random.normal(own_key, dims, jnp.float32)
    if cuts:
        drawn = drawn * steps_of(own_key, dims, cuts, -0.22, 0.18)
    return jnp.clip(raised(drawn, jax.random.fold_in(own_key, 3), *heavy), -limit, limit).astype(held_as)


def setup_inputs(seed: int = 0, part: int = 0) -> dict:
    keys = jax.random.split(jax.random.key(seed), 3)
    part_keys = jax.random.split(jax.random.fold_in(keys[2], part), 3)
    return {
        "activations": gaussian_with(part_keys[0], (TOKENS, ROWS), 1.0, 16.0, ((0, 64),), (0, 1, 64, 4.0)),
        "cotangents": scatter_about(part_keys[1], (TOKENS, FF), (max(1, TOK_DEV // (N_PAIR * N_DP))) ** -0.5, 1.75, ((0, 64),)),
    }


def reference(activations, cotangents):
    grad_sum = jnp.dot(activations.T, cotangents, preferred_element_type=jnp.float32)
    return (grad_sum / REPLICAS).astype(jnp.bfloat16)
```

```python
import jax
import jax.numpy as jnp
from jax import lax
from jax.sharding import Mesh
from jax.sharding import PartitionSpec as P

NEAR = ("pair", "x", "zl")
TOKENS = ("pair", "x", "zh", "zl")
SCALE = 2.0


def copies(x, axes, peers):
    return lax.all_to_all(
        jnp.broadcast_to(x, (peers, *x.shape)), axes, split_axis=0, concat_axis=0, tiled=True
    )


def local(activations, cotangents):
    near = lax.axis_size(NEAR)
    far = lax.axis_size("zh")
    in_plane = lax.axis_size(("x", "zl"))
    replicas = near * far
    partial_grad = lax.dot_general(
        activations, cotangents, (((0,), (0,)), ((), ())), preferred_element_type=jnp.float32
    )
    rows, cols = partial_grad.shape
    sent = (partial_grad * SCALE).astype(jnp.float16).reshape(near, rows // near, cols)
    arrived = lax.all_to_all(sent, NEAR, 0, 0, tiled=True)
    near_sum = jnp.sum(arrived.astype(jnp.float32), axis=0)
    parts = lax.all_to_all(near_sum.reshape(far, -1, cols), "zh", 0, 0, tiled=True)
    total = jnp.sum(parts, axis=0)
    own = (total * (1.0 / (SCALE * replicas))).astype(jnp.bfloat16)
    block = copies(own, "zh", far).reshape(-1, cols)
    return copies(block, ("x", "zl"), in_plane).reshape(-1, cols)


def solution(mesh):
    split = Mesh(
        mesh.devices.reshape(mesh.shape["pair"], 4, 4, 2, mesh.shape["ep"]),
        ("pair", "x", "zh", "zl", "ep"),
    )
    placed = (P(TOKENS, "ep"), P(TOKENS, "ep"))
    return jax.shard_map(
        local, mesh=split, in_specs=placed, out_specs=P("pair", "ep"), check_vma=False
    )
```

```python
import jax
import jax.numpy as jnp
from jax import lax
from jax.sharding import Mesh
from jax.sharding import PartitionSpec as P

NEAR = ("pair", "x")
TOKENS = ("pair", "x", "z")
SCALE = 2.0


def copies(x, axis):
    peers = lax.axis_size(axis)
    return lax.all_to_all(
        jnp.broadcast_to(x, (peers, *x.shape)), axis, split_axis=0, concat_axis=0, tiled=True
    )


def local(activations, cotangents):
    near = lax.axis_size(NEAR)
    far = lax.axis_size("z")
    replicas = near * far
    partial_grad = lax.dot_general(
        activations, cotangents, (((0,), (0,)), ((), ())), preferred_element_type=jnp.float32
    )
    rows, cols = partial_grad.shape
    sent = (partial_grad * SCALE).astype(jnp.float16).reshape(near, rows // near, cols)
    arrived = lax.all_to_all(sent, NEAR, 0, 0, tiled=True)
    near_sum = jnp.sum(arrived.astype(jnp.float32), axis=0)
    parts = lax.all_to_all(near_sum.reshape(far, -1, cols), "z", 0, 0, tiled=True)
    total = jnp.sum(parts, axis=0)
    own = (total * (1.0 / (SCALE * replicas))).astype(jnp.bfloat16)
    block = copies(own, "z").reshape(-1, cols)
    return copies(block, "x").reshape(-1, cols)


def solution(mesh):
    split = Mesh(
        mesh.devices.reshape(mesh.shape["pair"], 4, 8, mesh.shape["ep"]),
        ("pair", "x", "z", "ep"),
    )
    placed = (P(TOKENS, "ep"), P(TOKENS, "ep"))
    return jax.shard_map(
        local, mesh=split, in_specs=placed, out_specs=P("pair", "ep"), check_vma=False
    )
```

```python
import jax
import jax.numpy as jnp
from jax import lax
from jax.experimental import pallas as pl
from jax.experimental.pallas import tpu as pltpu
from jax.sharding import Mesh
from jax.sharding import PartitionSpec as P

NEAR = ("pair", "x", "zl")
TOKENS = ("pair", "x", "zh", "zl")
SCALE = 2.0
STAGGER_NS = 6000


def scale_kernel(late_ns, out):
    pl.delay(late_ns[0])
    out[...] = jnp.full(out.shape, SCALE, out.dtype)


def staggered_scale():
    late_ns = (lax.axis_index("ep") % 2) * STAGGER_NS
    return pl.pallas_call(
        scale_kernel,
        in_specs=[pl.BlockSpec(memory_space=pltpu.SMEM)],
        out_specs=pl.BlockSpec(memory_space=pltpu.VMEM),
        out_shape=jax.ShapeDtypeStruct((1, 128), jnp.float32),
        name="staggered_scale",
    )(late_ns.astype(jnp.int32).reshape(1))[0, 0]


def copies(x, axes, peers):
    return lax.all_to_all(
        jnp.broadcast_to(x, (peers, *x.shape)), axes, split_axis=0, concat_axis=0, tiled=True
    )


def local(activations, cotangents):
    near = lax.axis_size(NEAR)
    far = lax.axis_size("zh")
    in_plane = lax.axis_size(("x", "zl"))
    replicas = near * far
    partial_grad = lax.dot_general(
        activations, cotangents, (((0,), (0,)), ((), ())), preferred_element_type=jnp.float32
    )
    rows, cols = partial_grad.shape
    sent = (partial_grad * staggered_scale()).astype(jnp.float16).reshape(near, rows // near, cols)
    arrived = lax.all_to_all(sent, NEAR, 0, 0, tiled=True)
    near_sum = jnp.sum(arrived.astype(jnp.float32), axis=0)
    parts = lax.all_to_all(near_sum.reshape(far, -1, cols), "zh", 0, 0, tiled=True)
    total = jnp.sum(parts, axis=0)
    own = (total * (1.0 / (SCALE * replicas))).astype(jnp.bfloat16)
    block = copies(own, "zh", far).reshape(-1, cols)
    return copies(block, ("x", "zl"), in_plane).reshape(-1, cols)


def solution(mesh):
    split = Mesh(
        mesh.devices.reshape(mesh.shape["pair"], 4, 4, 2, mesh.shape["ep"]),
        ("pair", "x", "zh", "zl", "ep"),
    )
    placed = (P(TOKENS, "ep"), P(TOKENS, "ep"))
    return jax.shard_map(
        local, mesh=split, in_specs=placed, out_specs=P("pair", "ep"), check_vma=False
    )
```

```python
import jax
import jax.numpy as jnp
from jax import lax
from jax.sharding import Mesh
from jax.sharding import PartitionSpec as P

NEAR = ("pair", "x", "zl")
TOKENS = ("pair", "x", "zh", "zl")
SCALE = 2.0
LANES = 128
TOP = 15


def copies(x, axes, peers):
    return lax.all_to_all(
        jnp.broadcast_to(x, (peers, *x.shape)), axes, split_axis=0, concat_axis=0, tiled=True
    )


def coded(x):
    largest = jnp.maximum(jnp.max(jnp.abs(x)), 2.0**-100)
    k = jnp.ceil(jnp.log2(largest))
    u = x * jnp.exp2(-k)
    exponent = jnp.full((x.shape[0], LANES), k, jnp.float32)
    return jnp.concatenate([u * u * u * 2.0**TOP, exponent], axis=1).astype(jnp.float16)


def decoded(sent):
    code = sent[..., :-LANES].astype(jnp.float32)
    k = sent[..., -1:].astype(jnp.float32)
    return jnp.sign(code) * jnp.exp2((jnp.log2(jnp.abs(code)) - TOP) * (1.0 / 3.0) + k)


def local(activations, cotangents):
    near = lax.axis_size(NEAR)
    far = lax.axis_size("zh")
    in_plane = lax.axis_size(("x", "zl"))
    replicas = near * far
    partial_grad = lax.dot_general(
        activations, cotangents, (((0,), (0,)), ((), ())), preferred_element_type=jnp.float32
    )
    rows, cols = partial_grad.shape
    sent = (partial_grad * SCALE).astype(jnp.float16).reshape(near, rows // near, cols)
    arrived = lax.all_to_all(sent, NEAR, 0, 0, tiled=True)
    near_sum = jnp.sum(arrived.astype(jnp.float32), axis=0)
    total = jnp.sum(decoded(copies(coded(near_sum), "zh", far)), axis=0)
    own = (total * (1.0 / (SCALE * replicas))).astype(jnp.bfloat16)
    return copies(own, ("x", "zl"), in_plane).reshape(-1, cols)


def solution(mesh):
    split = Mesh(
        mesh.devices.reshape(mesh.shape["pair"], 4, 4, 2, mesh.shape["ep"]),
        ("pair", "x", "zh", "zl", "ep"),
    )
    placed = (P(TOKENS, "ep"), P(TOKENS, "ep"))
    return jax.shard_map(
        local, mesh=split, in_specs=placed, out_specs=P("pair", "ep"), check_vma=False
    )
```

```python
import itertools

import jax
import jax.numpy as jnp
from jax import lax
from jax.sharding import Mesh
from jax.sharding import PartitionSpec as P

SIZES = {"pair": 2, "x": 4, "zh": 4, "zl": 2}
NEAR = ("pair", "x")
ALONG_Z = ("zl", "zh")
TOKENS = ("pair", "x", "zh", "zl")
SLAB = ("yh", "core")
CORES = 2
SCALE = 2.0


def groups(axes_of_core):
    found = []
    for core, along in enumerate(axes_of_core):
        others = [axis for axis in SIZES if axis not in along]
        for rest in itertools.product(*(range(SIZES[axis]) for axis in others)):
            group = []
            for place in itertools.product(*(range(SIZES[axis]) for axis in along)):
                at = dict(zip((*others, *along), (*rest, *place)))
                index = 0
                for axis, size in SIZES.items():
                    index = index * size + at[axis]
                group.append(index * CORES + core)
            found.append(group)
    return found


def exchanged(x, axes_of_core):
    return lax.all_to_all(
        x, (*SIZES, "core"), 0, 0, axis_index_groups=groups(axes_of_core), tiled=True
    )


def copies(x, axes, peers):
    return lax.all_to_all(
        jnp.broadcast_to(x, (peers, *x.shape)), axes, split_axis=0, concat_axis=0, tiled=True
    )


def arranged(sent, near, far):
    cols = sent.shape[1]
    by_place = sent.reshape(near, far, -1, cols)
    mine = lax.axis_index("core") == 0
    return jnp.where(mine, by_place, jnp.swapaxes(by_place, 0, 1)).reshape(near, -1, cols)


def local(activations, cotangents):
    near = lax.axis_size(NEAR)
    far = lax.axis_size(ALONG_Z)
    replicas = near * far
    partial_grad = lax.dot_general(
        activations, cotangents, (((0,), (0,)), ((), ())), preferred_element_type=jnp.float32
    )
    cols = partial_grad.shape[1]
    sent = arranged((partial_grad * SCALE).astype(jnp.float16), near, far)
    first_sum = jnp.sum(exchanged(sent, (NEAR, ALONG_Z)).astype(jnp.float32), axis=0)
    parts = exchanged(first_sum.reshape(far, -1, cols), (ALONG_Z, NEAR))
    total = jnp.sum(parts, axis=0)
    own = (total * (1.0 / (SCALE * replicas))).astype(jnp.bfloat16)
    block = copies(own, "zh", lax.axis_size("zh")).reshape(-1, cols)
    return copies(block, ("x", "zl"), lax.axis_size(("x", "zl"))).reshape(-1, cols)


def solution(mesh):
    split = Mesh(
        mesh.devices.reshape(*SIZES.values(), mesh.shape["ep"] // CORES, CORES),
        (*SIZES, *SLAB),
    )
    placed = (P(TOKENS, SLAB), P(TOKENS, SLAB))
    return jax.shard_map(
        local, mesh=split, in_specs=placed, out_specs=P("pair", SLAB), check_vma=False
    )
```

```python
import itertools

import jax
import jax.numpy as jnp
from jax import lax
from jax.experimental import pallas as pl
from jax.experimental.pallas import tpu as pltpu
from jax.sharding import Mesh
from jax.sharding import PartitionSpec as P

SIZES = {"pair": 2, "x": 4, "zh": 4, "zl": 2}
NEAR = ("pair", "x")
ALONG_Z = ("zl", "zh")
TOKENS = ("pair", "x", "zh", "zl")
SLAB = ("yh", "core")
CORES = 2
SCALE = 2.0
CHUNKS = 2


def product_kernel(core, acts_hbm, cots_hbm, out, acts, cots, sems):
    near, far, _, cols = out.shape
    width = cols // CHUNKS
    loads = [pltpu.make_async_copy(acts_hbm, acts, sems.at[CHUNKS])]
    for i in range(CHUNKS):
        chunk = pl.ds(i * width, width)
        loads.append(pltpu.make_async_copy(cots_hbm.at[:, chunk], cots.at[:, chunk], sems.at[i]))
    for load in loads:
        load.start()

    def multiply(arrange):
        loads[0].wait()
        for i in range(CHUNKS):
            loads[i + 1].wait()
            chunk = pl.ds(i * width, width)
            part = lax.dot_general(
                acts[...],
                cots[:, chunk],
                (((0,), (0,)), ((), ())),
                preferred_element_type=jnp.float32,
            )
            out[:, :, :, chunk] = arrange(part.reshape(near, far, -1, width))

    @pl.when(core[0] == 0)
    def _():
        multiply(lambda rows: rows)

    @pl.when(core[0] != 0)
    def _():
        multiply(lambda rows: jnp.swapaxes(rows, 0, 1))


def product(activations, cotangents, near, far):
    tokens, rows = activations.shape
    cols = cotangents.shape[1]
    return pl.pallas_call(
        product_kernel,
        in_specs=[
            pl.BlockSpec(memory_space=pltpu.SMEM),
            pl.BlockSpec(memory_space=pltpu.HBM),
            pl.BlockSpec(memory_space=pltpu.HBM),
        ],
        out_specs=pl.BlockSpec(memory_space=pltpu.VMEM),
        out_shape=pltpu.VMEM((near, far, rows // (near * far), cols), jnp.float32),
        scratch_shapes=[
            pltpu.VMEM((tokens, rows), activations.dtype),
            pltpu.VMEM((tokens, cols), cotangents.dtype),
            pltpu.SemaphoreType.DMA((CHUNKS + 1,)),
        ],
        compiler_params=pltpu.CompilerParams(vmem_limit_bytes=20 * 2**20),
        name="product",
    )(
        lax.axis_index("core").astype(jnp.int32).reshape(1),
        pltpu.with_memory_space_constraint(activations, pltpu.HBM),
        pltpu.with_memory_space_constraint(cotangents, pltpu.HBM),
    )


def groups(axes_of_core):
    found = []
    for core, along in enumerate(axes_of_core):
        others = [axis for axis in SIZES if axis not in along]
        for rest in itertools.product(*(range(SIZES[axis]) for axis in others)):
            group = []
            for place in itertools.product(*(range(SIZES[axis]) for axis in along)):
                at = dict(zip((*others, *along), (*rest, *place)))
                index = 0
                for axis, size in SIZES.items():
                    index = index * size + at[axis]
                group.append(index * CORES + core)
            found.append(group)
    return found


def exchanged(x, axes_of_core):
    return lax.all_to_all(
        x, (*SIZES, "core"), 0, 0, axis_index_groups=groups(axes_of_core), tiled=True
    )


def copies(x, axes, peers):
    return lax.all_to_all(
        jnp.broadcast_to(x, (peers, *x.shape)), axes, split_axis=0, concat_axis=0, tiled=True
    )


def local(activations, cotangents):
    near = lax.axis_size(NEAR)
    far = lax.axis_size(ALONG_Z)
    replicas = near * far
    cols = cotangents.shape[1]
    partial_grad = product(activations, cotangents, near, far)
    sent = (partial_grad * SCALE).astype(jnp.float16).reshape(near, -1, cols)
    first_sum = jnp.sum(exchanged(sent, (NEAR, ALONG_Z)).astype(jnp.float32), axis=0)
    parts = exchanged(first_sum.reshape(far, -1, cols), (ALONG_Z, NEAR))
    total = jnp.sum(parts, axis=0)
    own = (total * (1.0 / (SCALE * replicas))).astype(jnp.bfloat16)
    block = copies(own, "zh", lax.axis_size("zh")).reshape(-1, cols)
    return copies(block, ("x", "zl"), lax.axis_size(("x", "zl"))).reshape(-1, cols)


def solution(mesh):
    split = Mesh(
        mesh.devices.reshape(*SIZES.values(), mesh.shape["ep"] // CORES, CORES),
        (*SIZES, *SLAB),
    )
    placed = (P(TOKENS, SLAB), P(TOKENS, SLAB))
    return jax.shard_map(
        local, mesh=split, in_specs=placed, out_specs=P("pair", SLAB), check_vma=False
    )
```

```python
import itertools

import jax
import jax.numpy as jnp
from jax import lax
from jax.experimental import pallas as pl
from jax.experimental.pallas import tpu as pltpu
from jax.sharding import Mesh
from jax.sharding import PartitionSpec as P

SIZES = {"pair": 2, "x": 4, "zh": 4, "zl": 2}
NEAR = ("pair", "x")
ALONG_Z = ("zl", "zh")
TOKENS = ("pair", "x", "zh", "zl")
SLAB = ("yh", "core")
CORES = 2
SCALE = 2.0
CHUNKS = 2
LATER_NS = 3000


def product_kernel(core, acts_hbm, cots_hbm, out, acts, cots, sems):
    near, far, _, cols = out.shape
    width = cols // CHUNKS
    loads = [pltpu.make_async_copy(acts_hbm, acts, sems.at[CHUNKS])]
    for i in range(CHUNKS):
        chunk = pl.ds(i * width, width)
        loads.append(pltpu.make_async_copy(cots_hbm.at[:, chunk], cots.at[:, chunk], sems.at[i]))
    for load in loads:
        load.start()

    def multiply(arrange):
        loads[0].wait()
        for i in range(CHUNKS):
            loads[i + 1].wait()
            chunk = pl.ds(i * width, width)
            part = lax.dot_general(
                acts[...],
                cots[:, chunk],
                (((0,), (0,)), ((), ())),
                preferred_element_type=jnp.float32,
            )
            out[:, :, :, chunk] = arrange(part.reshape(near, far, -1, width))

    @pl.when(core[0] == 0)
    def _():
        pl.delay(LATER_NS)
        multiply(lambda rows: rows)

    @pl.when(core[0] != 0)
    def _():
        multiply(lambda rows: jnp.swapaxes(rows, 0, 1))


def product(activations, cotangents, near, far):
    tokens, rows = activations.shape
    cols = cotangents.shape[1]
    return pl.pallas_call(
        product_kernel,
        in_specs=[
            pl.BlockSpec(memory_space=pltpu.SMEM),
            pl.BlockSpec(memory_space=pltpu.HBM),
            pl.BlockSpec(memory_space=pltpu.HBM),
        ],
        out_specs=pl.BlockSpec(memory_space=pltpu.VMEM),
        out_shape=pltpu.VMEM((near, far, rows // (near * far), cols), jnp.float32),
        scratch_shapes=[
            pltpu.VMEM((tokens, rows), activations.dtype),
            pltpu.VMEM((tokens, cols), cotangents.dtype),
            pltpu.SemaphoreType.DMA((CHUNKS + 1,)),
        ],
        compiler_params=pltpu.CompilerParams(vmem_limit_bytes=20 * 2**20),
        name="product",
    )(
        lax.axis_index("core").astype(jnp.int32).reshape(1),
        pltpu.with_memory_space_constraint(activations, pltpu.HBM),
        pltpu.with_memory_space_constraint(cotangents, pltpu.HBM),
    )


def groups(axes_of_core):
    found = []
    for core, along in enumerate(axes_of_core):
        others = [axis for axis in SIZES if axis not in along]
        for rest in itertools.product(*(range(SIZES[axis]) for axis in others)):
            group = []
            for place in itertools.product(*(range(SIZES[axis]) for axis in along)):
                at = dict(zip((*others, *along), (*rest, *place)))
                index = 0
                for axis, size in SIZES.items():
                    index = index * size + at[axis]
                group.append(index * CORES + core)
            found.append(group)
    return found


def exchanged(x, axes_of_core):
    return lax.all_to_all(
        x, (*SIZES, "core"), 0, 0, axis_index_groups=groups(axes_of_core), tiled=True
    )


def copies(x, axes, peers):
    return lax.all_to_all(
        jnp.broadcast_to(x, (peers, *x.shape)), axes, split_axis=0, concat_axis=0, tiled=True
    )


def local(activations, cotangents):
    near = lax.axis_size(NEAR)
    far = lax.axis_size(ALONG_Z)
    replicas = near * far
    cols = cotangents.shape[1]
    partial_grad = product(activations, cotangents, near, far)
    sent = (partial_grad * SCALE).astype(jnp.float16).reshape(near, -1, cols)
    first_sum = jnp.sum(exchanged(sent, (NEAR, ALONG_Z)).astype(jnp.float32), axis=0)
    parts = exchanged(first_sum.reshape(far, -1, cols), (ALONG_Z, NEAR))
    total = jnp.sum(parts, axis=0)
    own = (total * (1.0 / (SCALE * replicas))).astype(jnp.bfloat16)
    block = copies(own, "zh", lax.axis_size("zh")).reshape(-1, cols)
    return copies(block, ("x", "zl"), lax.axis_size(("x", "zl"))).reshape(-1, cols)


def solution(mesh):
    split = Mesh(
        mesh.devices.reshape(*SIZES.values(), mesh.shape["ep"] // CORES, CORES),
        (*SIZES, *SLAB),
    )
    placed = (P(TOKENS, SLAB), P(TOKENS, SLAB))
    return jax.shard_map(
        local, mesh=split, in_specs=placed, out_specs=P("pair", SLAB), check_vma=False
    )
```

```python
import functools
import itertools
import math

import jax
import jax.numpy as jnp
from jax import lax
from jax.experimental import pallas as pl
from jax.experimental.pallas import tpu as pltpu
from jax.sharding import Mesh
from jax.sharding import PartitionSpec as P

SIZES = {"pair": 2, "x": 4, "zh": 4, "zl": 2}
TOKENS = ("pair", "x", "zh", "zl")
SLAB = ("yh", "core")
CORES = 2
SCALE = 2.0
CHUNKS = 2
PLANS = (
    {"sums": (("x", "zl"), ("pair", "zh")), "blocks": (2, 8), "order": (1, 0)},
    {"sums": (("pair", "zl"), ("x",), ("zh",)), "blocks": (2, 4, 2), "order": (0, 2, 1)},
)
GATHERS = (("zh",), ("x", "zl"))


def product_kernel(blocks, order, acts_hbm, cots_hbm, out, acts, cots, sems):
    cols = out.shape[-1]
    width = cols // CHUNKS
    loads = [pltpu.make_async_copy(acts_hbm, acts, sems.at[CHUNKS])]
    for i in range(CHUNKS):
        chunk = pl.ds(i * width, width)
        loads.append(pltpu.make_async_copy(cots_hbm.at[:, chunk], cots.at[:, chunk], sems.at[i]))
    for load in loads:
        load.start()
    loads[0].wait()
    for i in range(CHUNKS):
        loads[i + 1].wait()
        at = i * width
        part = lax.dot_general(
            acts[...],
            cots[:, at : at + width],
            (((0,), (0,)), ((), ())),
            preferred_element_type=jnp.float32,
        )
        rows = part.shape[0]
        piece = rows // math.prod(blocks)
        place = {}
        for n, index in enumerate(itertools.product(*(range(b) for b in blocks))):
            moved = 0
            for axis in order:
                moved = moved * blocks[axis] + index[axis]
            place[n] = moved
        for n, moved in place.items():
            out[moved * piece : (moved + 1) * piece, at : at + width] = part[
                n * piece : (n + 1) * piece
            ]


def product(activations, cotangents, plan):
    tokens, rows = activations.shape
    cols = cotangents.shape[1]
    return pl.pallas_call(
        functools.partial(product_kernel, plan["blocks"], plan["order"]),
        in_specs=[pl.BlockSpec(memory_space=pltpu.HBM)] * 2,
        out_specs=pl.BlockSpec(memory_space=pltpu.VMEM),
        out_shape=pltpu.VMEM((rows, cols), jnp.float32),
        scratch_shapes=[
            pltpu.VMEM((tokens, rows), activations.dtype),
            pltpu.VMEM((tokens, cols), cotangents.dtype),
            pltpu.SemaphoreType.DMA((CHUNKS + 1,)),
        ],
        compiler_params=pltpu.CompilerParams(vmem_limit_bytes=20 * 2**20),
        name="product",
    )(
        pltpu.with_memory_space_constraint(activations, pltpu.HBM),
        pltpu.with_memory_space_constraint(cotangents, pltpu.HBM),
    )


def groups(along):
    found = []
    for core in range(CORES):
        others = [axis for axis in SIZES if axis not in along]
        for rest in itertools.product(*(range(SIZES[axis]) for axis in others)):
            group = []
            for place in itertools.product(*(range(SIZES[axis]) for axis in along)):
                at = dict(zip((*others, *along), (*rest, *place)))
                z = at["zh"] * SIZES["zl"] + at["zl"] + core
                at["zh"], at["zl"] = divmod(z % (SIZES["zh"] * SIZES["zl"]), SIZES["zl"])
                index = 0
                for axis, size in SIZES.items():
                    index = index * size + at[axis]
                group.append(index * CORES + core)
            found.append(group)
    return found


def exchanged(x, along):
    return lax.all_to_all(
        x, (*SIZES, "core"), 0, 0, axis_index_groups=groups(along), tiled=True
    )


def peers(along):
    return math.prod(SIZES[axis] for axis in along)


def branch(plan):
    def run(activations, cotangents):
        cols = cotangents.shape[1]
        rows = (product(activations, cotangents, plan) * SCALE).astype(jnp.float16)
        for along in plan["sums"]:
            arrived = exchanged(rows.reshape(peers(along), -1, cols), along)
            rows = jnp.sum(arrived.astype(jnp.float32), axis=0)
        block = (rows * (1.0 / (SCALE * math.prod(SIZES.values())))).astype(jnp.bfloat16)
        for along in GATHERS:
            block = exchanged(jnp.broadcast_to(block, (peers(along), *block.shape)), along)
            block = block.reshape(-1, cols)
        return block

    return run


def local(activations, cotangents):
    first, second = (branch(plan) for plan in PLANS)
    return lax.cond(lax.axis_index("core") == 0, first, second, activations, cotangents)


def solution(mesh):
    split = Mesh(
        mesh.devices.reshape(*SIZES.values(), mesh.shape["ep"] // CORES, CORES),
        (*SIZES, *SLAB),
    )
    placed = (P(TOKENS, SLAB), P(TOKENS, SLAB))
    return jax.shard_map(
        local, mesh=split, in_specs=placed, out_specs=P("pair", SLAB), check_vma=False
    )
```

```python
import functools
import itertools
import math

import jax
import jax.numpy as jnp
from jax import lax
from jax.experimental import pallas as pl
from jax.experimental.pallas import tpu as pltpu
from jax.sharding import Mesh
from jax.sharding import PartitionSpec as P

SIZES = {"pair": 2, "x": 4, "zh": 4, "zl": 2}
TOKENS = ("pair", "x", "zh", "zl")
SLAB = ("yh", "core")
CORES = 2
SCALE = 2.0
CHUNKS = 2
PLANS = (
    {
        "sums": (("x", "zl"), ("pair", "zh")),
        "whole": (),
        "gathers": (("zh",), ("x", "zl")),
        "blocks": (2, 8),
        "order": (1, 0),
    },
    {
        "sums": (("pair", "zl"), ("x",)),
        "whole": (("zh",),),
        "gathers": (("x", "zl"),),
        "blocks": (2, 4, 2),
        "order": (0, 2, 1),
    },
)


def product_kernel(blocks, order, acts_hbm, cots_hbm, out, acts, cots, sems):
    cols = out.shape[-1]
    width = cols // CHUNKS
    loads = [pltpu.make_async_copy(acts_hbm, acts, sems.at[CHUNKS])]
    for i in range(CHUNKS):
        chunk = pl.ds(i * width, width)
        loads.append(pltpu.make_async_copy(cots_hbm.at[:, chunk], cots.at[:, chunk], sems.at[i]))
    for load in loads:
        load.start()
    loads[0].wait()
    for i in range(CHUNKS):
        loads[i + 1].wait()
        at = i * width
        part = lax.dot_general(
            acts[...],
            cots[:, at : at + width],
            (((0,), (0,)), ((), ())),
            preferred_element_type=jnp.float32,
        )
        rows = part.shape[0]
        piece = rows // math.prod(blocks)
        place = {}
        for n, index in enumerate(itertools.product(*(range(b) for b in blocks))):
            moved = 0
            for axis in order:
                moved = moved * blocks[axis] + index[axis]
            place[n] = moved
        for n, moved in place.items():
            out[moved * piece : (moved + 1) * piece, at : at + width] = part[
                n * piece : (n + 1) * piece
            ]


def product(activations, cotangents, plan):
    tokens, rows = activations.shape
    cols = cotangents.shape[1]
    return pl.pallas_call(
        functools.partial(product_kernel, plan["blocks"], plan["order"]),
        in_specs=[pl.BlockSpec(memory_space=pltpu.HBM)] * 2,
        out_specs=pl.BlockSpec(memory_space=pltpu.VMEM),
        out_shape=pltpu.VMEM((rows, cols), jnp.float32),
        scratch_shapes=[
            pltpu.VMEM((tokens, rows), activations.dtype),
            pltpu.VMEM((tokens, cols), cotangents.dtype),
            pltpu.SemaphoreType.DMA((CHUNKS + 1,)),
        ],
        compiler_params=pltpu.CompilerParams(vmem_limit_bytes=20 * 2**20),
        name="product",
    )(
        pltpu.with_memory_space_constraint(activations, pltpu.HBM),
        pltpu.with_memory_space_constraint(cotangents, pltpu.HBM),
    )


def groups(along):
    found = []
    for core in range(CORES):
        others = [axis for axis in SIZES if axis not in along]
        for rest in itertools.product(*(range(SIZES[axis]) for axis in others)):
            group = []
            for place in itertools.product(*(range(SIZES[axis]) for axis in along)):
                at = dict(zip((*others, *along), (*rest, *place)))
                z = at["zh"] * SIZES["zl"] + at["zl"] + core
                at["zh"], at["zl"] = divmod(z % (SIZES["zh"] * SIZES["zl"]), SIZES["zl"])
                index = 0
                for axis, size in SIZES.items():
                    index = index * size + at[axis]
                group.append(index * CORES + core)
            found.append(group)
    return found


def exchanged(x, along):
    return lax.all_to_all(
        x, (*SIZES, "core"), 0, 0, axis_index_groups=groups(along), tiled=True
    )


def peers(along):
    return math.prod(SIZES[axis] for axis in along)


def copies(x, along):
    return exchanged(jnp.broadcast_to(x, (peers(along), *x.shape)), along)


def branch(plan):
    def run(activations, cotangents):
        cols = cotangents.shape[1]
        rows = (product(activations, cotangents, plan) * SCALE).astype(jnp.float16)
        for along in plan["sums"]:
            arrived = exchanged(rows.reshape(peers(along), -1, cols), along)
            rows = jnp.sum(arrived.astype(jnp.float32), axis=0)
        for along in plan["whole"]:
            rows = jnp.sum(copies(rows, along), axis=0)
        block = (rows * (1.0 / (SCALE * math.prod(SIZES.values())))).astype(jnp.bfloat16)
        for along in plan["gathers"]:
            block = copies(block, along).reshape(-1, cols)
        return block

    return run


def local(activations, cotangents):
    first, second = (branch(plan) for plan in PLANS)
    return lax.cond(lax.axis_index("core") == 0, first, second, activations, cotangents)


def solution(mesh):
    split = Mesh(
        mesh.devices.reshape(*SIZES.values(), mesh.shape["ep"] // CORES, CORES),
        (*SIZES, *SLAB),
    )
    placed = (P(TOKENS, SLAB), P(TOKENS, SLAB))
    return jax.shard_map(
        local, mesh=split, in_specs=placed, out_specs=P("pair", SLAB), check_vma=False
    )
```

```python
import functools
import itertools
import math

import jax
import jax.numpy as jnp
from jax import lax
from jax.experimental import pallas as pl
from jax.experimental.pallas import tpu as pltpu
from jax.sharding import Mesh
from jax.sharding import PartitionSpec as P

SIZES = {"pair": 2, "x": 4, "zh": 4, "zl": 2}
TOKENS = ("pair", "x", "zh", "zl")
SLAB = ("yh", "core")
CORES = 2
SCALE = 2.0
CHUNKS = 2
PLANS = (
    {"sums": (("x", "zl"), ("pair", "zh")), "blocks": (2, 8), "order": (1, 0), "gathers": (("zh",), ("x", "zl"))},
    {"sums": (("pair", "zl"), ("x",), ("zh",)), "blocks": (2, 4, 2), "order": (0, 2, 1), "gathers": (("zl", "zh"), ("x",))},
)


def product_kernel(blocks, order, acts_hbm, cots_hbm, out, acts, cots, sems):
    cols = out.shape[-1]
    width = cols // CHUNKS
    loads = [pltpu.make_async_copy(acts_hbm, acts, sems.at[CHUNKS])]
    for i in range(CHUNKS):
        chunk = pl.ds(i * width, width)
        loads.append(pltpu.make_async_copy(cots_hbm.at[:, chunk], cots.at[:, chunk], sems.at[i]))
    for load in loads:
        load.start()
    loads[0].wait()
    for i in range(CHUNKS):
        loads[i + 1].wait()
        at = i * width
        part = lax.dot_general(
            acts[...],
            cots[:, at : at + width],
            (((0,), (0,)), ((), ())),
            preferred_element_type=jnp.float32,
        )
        rows = part.shape[0]
        piece = rows // math.prod(blocks)
        place = {}
        for n, index in enumerate(itertools.product(*(range(b) for b in blocks))):
            moved = 0
            for axis in order:
                moved = moved * blocks[axis] + index[axis]
            place[n] = moved
        for n, moved in place.items():
            out[moved * piece : (moved + 1) * piece, at : at + width] = part[
                n * piece : (n + 1) * piece
            ]


def product(activations, cotangents, plan):
    tokens, rows = activations.shape
    cols = cotangents.shape[1]
    return pl.pallas_call(
        functools.partial(product_kernel, plan["blocks"], plan["order"]),
        in_specs=[pl.BlockSpec(memory_space=pltpu.HBM)] * 2,
        out_specs=pl.BlockSpec(memory_space=pltpu.VMEM),
        out_shape=pltpu.VMEM((rows, cols), jnp.float32),
        scratch_shapes=[
            pltpu.VMEM((tokens, rows), activations.dtype),
            pltpu.VMEM((tokens, cols), cotangents.dtype),
            pltpu.SemaphoreType.DMA((CHUNKS + 1,)),
        ],
        compiler_params=pltpu.CompilerParams(vmem_limit_bytes=20 * 2**20),
        name="product",
    )(
        pltpu.with_memory_space_constraint(activations, pltpu.HBM),
        pltpu.with_memory_space_constraint(cotangents, pltpu.HBM),
    )


def groups(along):
    found = []
    for core in range(CORES):
        others = [axis for axis in SIZES if axis not in along]
        for rest in itertools.product(*(range(SIZES[axis]) for axis in others)):
            group = []
            for place in itertools.product(*(range(SIZES[axis]) for axis in along)):
                at = dict(zip((*others, *along), (*rest, *place)))
                z = at["zh"] * SIZES["zl"] + at["zl"] + core
                at["zh"], at["zl"] = divmod(z % (SIZES["zh"] * SIZES["zl"]), SIZES["zl"])
                index = 0
                for axis, size in SIZES.items():
                    index = index * size + at[axis]
                group.append(index * CORES + core)
            found.append(group)
    return found


def exchanged(x, along):
    return lax.all_to_all(
        x, (*SIZES, "core"), 0, 0, axis_index_groups=groups(along), tiled=True
    )


def peers(along):
    return math.prod(SIZES[axis] for axis in along)


def branch(plan):
    def run(activations, cotangents):
        cols = cotangents.shape[1]
        rows = (product(activations, cotangents, plan) * SCALE).astype(jnp.float16)
        for along in plan["sums"]:
            arrived = exchanged(rows.reshape(peers(along), -1, cols), along)
            rows = jnp.sum(arrived.astype(jnp.float32), axis=0)
        block = (rows * (1.0 / (SCALE * math.prod(SIZES.values())))).astype(jnp.bfloat16)
        for along in plan["gathers"]:
            block = exchanged(jnp.broadcast_to(block, (peers(along), *block.shape)), along)
            block = block.reshape(-1, cols)
        return block

    return run


def local(activations, cotangents):
    first, second = (branch(plan) for plan in PLANS)
    return lax.cond(lax.axis_index("core") == 0, first, second, activations, cotangents)


def solution(mesh):
    split = Mesh(
        mesh.devices.reshape(*SIZES.values(), mesh.shape["ep"] // CORES, CORES),
        (*SIZES, *SLAB),
    )
    placed = (P(TOKENS, SLAB), P(TOKENS, SLAB))
    return jax.shard_map(
        local, mesh=split, in_specs=placed, out_specs=P("pair", SLAB), check_vma=False
    )
```
